16 devices in a mesh: dp: 2 (over z), ep: 8 (over y, x, core).
Axes of the slice: x: 2, y: 2, z: 2, core: 2. Of those that a mesh axis runs over, the one named last changes fastest.
Arguments:
- x_tokens: bfloat16 [131072, 768], P(('dp', 'ep'))
- modality: int32 [131072], P(('dp', 'ep'))
- router: float32 [768, 32], replicated
- expert_ids: int32 [131072], P(('dp', 'ep'))
- priority: int32 [131072], P(('dp', 'ep'))
- w_in: bfloat16 [32, 768, 3072], P('ep')
- b_in: bfloat16 [32, 3072], P('ep')
- w_out: bfloat16 [32, 3072, 768], P('ep')
- b_out: bfloat16 [32, 768], P('ep')
- dy_out: bfloat16 [131072, 768], P(('dp', 'ep'))
Outputs:
- output 1: bfloat16 [131072, 768], P(('dp', 'ep'))
- output 2: float32 [], replicated
- output 3: bfloat16 [131072, 768], P(('dp', 'ep'))
- output 4: float32 [768, 32], replicated
- output 5: bfloat16 [32, 768, 3072], P('ep')
- output 6: bfloat16 [32, 3072], P('ep')
- output 7: bfloat16 [32, 3072, 768], P('ep')
- output 8: bfloat16 [32, 768], P('ep')
All inputs are finite; a program needn't handle non-finite values.
Results may differ from the reference program's by a relative error of at most 0.00946785.
Values are sent between devices in bfloat16 or wider.
A program may use at most 1 GiB of HBM per device.

```python
import jax
import jax.numpy as jnp
from jax import lax

TOKENS = 8192
WIDTH = 768
HIDDEN = 3072
EXPERTS = 32
GROUPS = 16


def setup_inputs(seed: int = 0) -> dict:
    total_tokens = TOKENS * GROUPS
    key_set = jax.random.split(jax.random.key(seed), 16)
    local_index = jnp.arange(TOKENS)[None, :]
    text_pct = jax.random.randint(key_set[0], (GROUPS, 1), 5, 41)
    modality = (jax.random.randint(key_set[1], (GROUPS, TOKENS), 0, 100) < text_pct).astype(jnp.int32)
    modality = jnp.where(local_index == 0, 0, jnp.where(local_index == 1, 1, modality))
    hot_base = jax.random.randint(key_set[2], (GROUPS, 1), 0, EXPERTS)
    hot_pick = (hot_base + jax.random.randint(key_set[3], (GROUPS, TOKENS), 0, 4)) % EXPERTS
    spread_pick = jax.random.randint(key_set[4], (GROUPS, TOKENS), 0, EXPERTS)
    use_hot = (modality == 1) & (jax.random.randint(key_set[5], (GROUPS, TOKENS), 0, 4) < 3)
    expert_ids = jnp.where(local_index < EXPERTS, local_index, jnp.where(use_hot, hot_pick, spread_pick))
    priority = jax.vmap(lambda perm_key: jax.random.permutation(perm_key, TOKENS))(jax.random.split(key_set[6], GROUPS))
    router = jax.random.normal(key_set[7], (WIDTH, EXPERTS), jnp.float32) * WIDTH ** -0.5
    boost_dir = router.T / jnp.sum(router * router, axis=0)[:, None]
    expert_onehot = (expert_ids.reshape(total_tokens, 1) == jnp.arange(EXPERTS)[None, :]).astype(jnp.float32)
    base_noise = jax.random.normal(key_set[8], (GROUPS, TOKENS, WIDTH), jnp.float32)
    group_shift = 0.5 * jax.random.normal(key_set[9], (GROUPS, 1, WIDTH), jnp.float32)
    text_shift = 0.5 * jax.random.normal(key_set[10], (WIDTH,), jnp.float32)
    x_tokens = (base_noise + group_shift + modality[:, :, None] * text_shift).reshape(total_tokens, WIDTH)
    x_tokens = x_tokens + 4.0 * jnp.dot(expert_onehot, boost_dir)
    w_in = jax.random.normal(key_set[11], (EXPERTS, WIDTH, HIDDEN), jnp.float32) * WIDTH ** -0.5
    b_in = 0.5 * jax.random.normal(key_set[12], (EXPERTS, HIDDEN), jnp.float32)
    w_out = jax.random.normal(key_set[13], (EXPERTS, HIDDEN, WIDTH), jnp.float32) * HIDDEN ** -0.5
    b_out = 0.5 * jax.random.normal(key_set[14], (EXPERTS, WIDTH), jnp.float32)
    dy_out = jax.random.normal(key_set[15], (total_tokens, WIDTH), jnp.float32) * (total_tokens * WIDTH) ** -0.5
    return dict(
        x_tokens=x_tokens.astype(jnp.bfloat16),
        modality=modality.reshape(total_tokens).astype(jnp.int32),
        router=router,
        expert_ids=expert_ids.reshape(total_tokens).astype(jnp.int32),
        priority=priority.reshape(total_tokens).astype(jnp.int32),
        w_in=w_in.astype(jnp.bfloat16),
        b_in=b_in.astype(jnp.bfloat16),
        w_out=w_out.astype(jnp.bfloat16),
        b_out=b_out.astype(jnp.bfloat16),
        dy_out=dy_out.astype(jnp.bfloat16),
    )


def route_group(expert_ids, priority):
    capacity = TOKENS // EXPERTS
    sort_order = jnp.argsort(expert_ids * TOKENS + priority)
    sorted_rank = jnp.argsort(sort_order)
    counts = jnp.sum((expert_ids[:, None] == jnp.arange(EXPERTS)[None, :]).astype(jnp.int32), axis=0)
    starts = jnp.cumsum(counts) - counts
    slot_rank = jnp.arange(capacity)
    slot_token = sort_order[jnp.minimum(starts[:, None] + slot_rank[None, :], TOKENS - 1)]
    slot_valid = slot_rank[None, :] < counts[:, None]
    position = sorted_rank - starts[expert_ids]
    return slot_token, slot_valid, position


def expert_block(operands):
    slot_rows, w_first, b_first, w_second, b_second = operands
    act_in = jnp.dot(slot_rows, w_first, preferred_element_type=jnp.float32) + b_first.astype(jnp.float32)
    hidden = jax.nn.gelu(act_in).astype(jnp.bfloat16)
    expert_out = jnp.dot(hidden, w_second, preferred_element_type=jnp.float32) + b_second.astype(jnp.float32)
    return expert_out.astype(jnp.bfloat16)


def reference(x_tokens, modality, router, expert_ids, priority, w_in, b_in, w_out, b_out, dy_out):
    total_tokens = x_tokens.shape[0]
    groups = total_tokens // TOKENS
    capacity = TOKENS // EXPERTS
    slot_token, slot_valid, position = jax.vmap(route_group)(expert_ids.reshape(groups, TOKENS), priority.reshape(groups, TOKENS))
    group_base = jnp.arange(groups)[:, None, None] * TOKENS
    slot_global = jnp.transpose(slot_token + group_base, (1, 0, 2)).reshape(EXPERTS, groups * capacity)
    valid_global = jnp.transpose(slot_valid, (1, 0, 2)).reshape(EXPERTS, groups * capacity, 1)
    position = position.reshape(total_tokens)
    keep_mask = (position < capacity)[:, None]
    group_of = jnp.arange(total_tokens) // TOKENS
    token_slot = expert_ids * (groups * capacity) + group_of * capacity + jnp.minimum(position, capacity - 1)
    expert_onehot = (expert_ids[:, None] == jnp.arange(EXPERTS)[None, :]).astype(jnp.float32)
    mod_mask = jnp.stack([modality == 0, modality == 1]).astype(jnp.float32)
    mod_count = jnp.sum(mod_mask, axis=1)

    def forward(x_in, router_in, w_first, b_first, w_second, b_second):
        logits = jnp.dot(x_in.astype(jnp.float32), router_in)
        log_probs = jax.nn.log_softmax(logits, axis=-1)
        router_probs = jnp.exp(log_probs)
        gate_prob = jnp.sum(router_probs * expert_onehot, axis=-1, keepdims=True)
        entropy = -jnp.sum(router_probs * log_probs, axis=-1)
        mean_probs = jnp.dot(mod_mask, router_probs) / mod_count[:, None]
        aux_loss = jnp.sum(jnp.dot(mod_mask, entropy) / mod_count) + jnp.sum(mean_probs * jnp.log(mean_probs))
        gathered = jnp.where(valid_global, x_in[slot_global], 0.0).astype(x_in.dtype)
        expert_out = lax.map(jax.checkpoint(expert_block), (gathered, w_first, b_first, w_second, b_second))
        y_tok = expert_out.reshape(EXPERTS * groups * capacity, WIDTH)[token_slot]
        out_tokens = jnp.where(keep_mask, gate_prob * y_tok.astype(jnp.float32), 0.0).astype(jnp.bfloat16)
        return out_tokens, aux_loss

    (out_tokens, aux_loss), pullback = jax.vjp(forward, x_tokens, router, w_in, b_in, w_out, b_out)
    dx_tokens, d_router, d_w_in, d_b_in, d_w_out, d_b_out = pullback((dy_out, jnp.ones_like(aux_loss)))
    return out_tokens, aux_loss, dx_tokens, d_router, d_w_in, d_b_in, d_w_out, d_b_out
```

```python
import functools

import jax
import jax.numpy as jnp
from jax import lax
from jax.experimental import pallas as pl
from jax.experimental.pallas import tpu as pltpu
from jax.sharding import PartitionSpec as P


ALL_AXES = ("dp", "ep")
PAD_ROWS = 8


def route_tokens(expert_ids, priority, num_experts, capacity, ep_size):
    num_tokens = expert_ids.shape[0]
    local_experts = num_experts // ep_size
    num_slots = num_experts * capacity
    token_iota = jnp.arange(num_tokens, dtype=jnp.int32)
    slot_iota = jnp.arange(num_slots, dtype=jnp.int32)
    span = num_tokens + capacity
    key_tok = expert_ids * span + priority
    key_fill = (slot_iota // capacity) * span + num_tokens + slot_iota % capacity
    item = jnp.concatenate([token_iota, jnp.full((num_slots,), num_tokens, jnp.int32)])
    sorted_key, sorted_item = lax.sort((jnp.concatenate([key_tok, key_fill]), item), num_keys=1, is_stable=False)
    expert_range = jnp.arange(num_experts, dtype=jnp.int32)
    counts = jnp.sum((expert_ids[:, None] == expert_range[None, :]).astype(jnp.int32), axis=0) + capacity
    expert_of = sorted_key // span
    begin = jnp.sum(jnp.where(expert_range[:, None] < expert_of[None, :], counts[:, None], 0), axis=0)
    position = jnp.arange(num_tokens + num_slots, dtype=jnp.int32) - begin
    keep = position < capacity
    slot = ((expert_of % local_experts) * ep_size + expert_of // local_experts) * capacity + jnp.minimum(position, capacity - 1)
    spread = jnp.where(keep, slot, num_slots)
    _, slot_item = lax.sort((spread, sorted_item), num_keys=1, is_stable=False)
    slot_token = slot_item[:num_slots]
    code = slot * 2 + keep.astype(jnp.int32)
    _, token_code = lax.sort((sorted_item, code), num_keys=1, is_stable=False)
    token_code = token_code[:num_tokens]
    return slot_token, token_code // 2, (token_code % 2) == 1


def router_forward(x_loc, modality, router, expert_ids):
    num_experts = router.shape[1]
    logits = jnp.dot(x_loc, router, precision=lax.Precision.HIGHEST, preferred_element_type=jnp.float32)
    log_probs = jax.nn.log_softmax(logits, axis=-1)
    router_probs = jnp.exp(log_probs)
    expert_onehot = (expert_ids[:, None] == jnp.arange(num_experts)[None, :]).astype(jnp.float32)
    gate_prob = jnp.sum(router_probs * expert_onehot, axis=-1)
    mod_mask = jnp.stack([modality == 0, modality == 1]).astype(jnp.float32)
    entropy = -jnp.sum(router_probs * log_probs, axis=-1)
    local_stats = jnp.concatenate([jnp.dot(mod_mask, router_probs), jnp.dot(mod_mask, entropy)[:, None], jnp.sum(mod_mask, axis=1, keepdims=True)], axis=1)
    return log_probs, router_probs, expert_onehot, gate_prob, mod_mask, local_stats


def aux_from_stats(stats, num_experts):
    mod_count = stats[:, num_experts + 1]
    mean_probs = stats[:, :num_experts] / mod_count[:, None]
    aux_loss = jnp.sum(stats[:, num_experts] / mod_count) + jnp.sum(mean_probs * jnp.log(mean_probs))
    return aux_loss, mean_probs, mod_count


def router_backward(x_loc, router, log_probs, router_probs, expert_onehot, mod_mask, mean_probs, mod_count, d_gate):
    inv_count = jnp.dot(1.0 / mod_count, mod_mask)
    global_part = jnp.einsum("mt,me->te", mod_mask, jnp.log(mean_probs) / mod_count[:, None])
    d_probs = expert_onehot * d_gate[:, None] + global_part - log_probs * inv_count[:, None]
    d_logits = router_probs * (d_probs - jnp.sum(d_probs * router_probs, axis=-1, keepdims=True))
    d_router_part = jnp.einsum("tw,te->we", x_loc, d_logits, precision=lax.Precision.HIGHEST, preferred_element_type=jnp.float32)
    dx_router = jnp.einsum("te,we->tw", d_logits, router, precision=lax.Precision.HIGHEST, preferred_element_type=jnp.float32)
    return d_router_part, dx_router.astype(jnp.bfloat16)


GELU_A = 0.7978845608028654
GELU_B = 0.044715 * GELU_A
NT = (((1,), (1,)), ((), ()))
NN = (((1,), (0,)), ((), ()))


def mm(lhs, rhs, dims=NN):
    return lax.dot_general(lhs, rhs, dims, preferred_element_type=jnp.float32)


def gelu_and_slope(act):
    sq = act * act
    gate = 0.5 * jnp.tanh(act * (GELU_B * sq + GELU_A)) + 0.5
    value = act * gate
    slope = gate + value * (1.0 - gate) * (6.0 * GELU_B * sq + 2.0 * GELU_A)
    return value, slope


def act_tile(x_rows, d_rows, w_in, bias, w_out):
    act = mm(x_rows, w_in) + bias
    d_hidden = mm(d_rows, w_out, NT).astype(jnp.bfloat16).astype(jnp.float32)
    value, slope = gelu_and_slope(act)
    return value.astype(jnp.bfloat16), d_hidden * slope


def own_kernel(tile, sub, rows_ref, w_in_ref, b_in_ref, w_out_ref, b_out_ref, both_ref, hidden_ref, dact_ref, dbias_ref):
    count = rows_ref.shape[0]
    width = w_in_ref.shape[0]
    hidden_size = w_in_ref.shape[1]

    @pl.when(pl.program_id(0) == 0)
    def _():
        dbias_ref[...] = jnp.zeros_like(dbias_ref)

    def hidden_step(step, carry):
        for part in range(tile // sub):
            cols = pl.ds(pl.multiple_of(step * tile + part * sub, sub), sub)
            total = jnp.zeros((1, sub), jnp.float32)
            for start in range(0, count, sub):
                block = slice(start, start + sub)
                value, d_act = act_tile(rows_ref[block, :width], rows_ref[block, width:], w_in_ref[:, cols], b_in_ref[:, cols].astype(jnp.float32), w_out_ref[cols, :])
                hidden_ref[block, cols] = value
                dact_ref[block, cols] = d_act.astype(jnp.bfloat16)
                total = total + jnp.sum(d_act, axis=0, keepdims=True)
            dbias_ref[:, cols] += total
        return carry

    lax.fori_loop(0, hidden_size // tile, hidden_step, 0)

    def out_step(step, carry):
        cols = pl.ds(pl.multiple_of(step * sub, sub), sub)
        back = pl.ds(pl.multiple_of(width + step * sub, sub), sub)
        both_ref[:, cols] = (mm(hidden_ref[...], w_out_ref[:, cols]) + b_out_ref[:, cols].astype(jnp.float32)).astype(jnp.bfloat16)
        both_ref[:, back] = mm(dact_ref[...], w_in_ref[cols, :], NT).astype(jnp.bfloat16)
        return carry

    lax.fori_loop(0, width // sub, out_step, 0)


def own_call(index, rows, w_in, b_in, w_out, b_out, block=512):
    num_rows, wide = rows.shape
    width = wide // 2
    hidden_size = w_in.shape[2]
    whole = lambda shape: pl.BlockSpec((None,) + shape, lambda i: (index, 0, 0), pipeline_mode=pl.Buffered(1))
    flops = 8 * num_rows * width * hidden_size
    return pl.pallas_call(
        functools.partial(own_kernel, 512, 256),
        grid=(num_rows // block,),
        in_specs=[
            pl.BlockSpec((block, wide), lambda i: (i, 0)),
            whole((width, hidden_size)),
            whole((1, hidden_size)),
            whole((hidden_size, width)),
            whole((1, width)),
        ],
        out_specs=[
            pl.BlockSpec((block, wide), lambda i: (i, 0)),
            pl.BlockSpec((block, hidden_size), lambda i: (i, 0)),
            pl.BlockSpec((block, hidden_size), lambda i: (i, 0)),
            pl.BlockSpec((1, hidden_size), lambda i: (0, 0)),
        ],
        out_shape=[
            jax.ShapeDtypeStruct((num_rows, wide), jnp.bfloat16),
            jax.ShapeDtypeStruct((num_rows, hidden_size), jnp.bfloat16),
            jax.ShapeDtypeStruct((num_rows, hidden_size), jnp.bfloat16),
            jax.ShapeDtypeStruct((1, hidden_size), jnp.float32),
        ],
        compiler_params=pltpu.CompilerParams(dimension_semantics=("arbitrary",), vmem_limit_bytes=60 * 2**20),
        cost_estimate=pl.CostEstimate(flops=flops, bytes_accessed=8 * num_rows * hidden_size, transcendentals=num_rows * hidden_size),
        name="expert_own",
    )(rows, w_in, b_in[:, None, :], w_out, b_out[:, None, :])


def grad_kernel(sub, own_ref, other_ref, hidden_ref, dact_ref, dbias_ref, w_in_ref, b_in_ref, w_out_ref, *refs):
    dw_in_ref, db_in_ref, dw_out_ref, db_out_ref, xt_ref, dt_ref, h_ref, a_ref = refs[-8:]
    half = own_ref.shape[0]
    width = own_ref.shape[1] // 2
    tile = w_in_ref.shape[1]

    @pl.when(pl.program_id(0) == 0)
    def _():
        def flip(step, total):
            for ref, base in ((own_ref, 0), (other_ref, half)):
                block = pl.ds(pl.multiple_of(step * sub, sub), sub)
                cols = pl.ds(pl.multiple_of(base + step * sub, sub), sub)
                d_rows = ref[block, width:]
                xt_ref[:, cols] = ref[block, :width].T
                dt_ref[:, cols] = d_rows.T
                total = total + jnp.sum(d_rows.astype(jnp.float32), axis=0, keepdims=True)
            return total

        total = lax.fori_loop(0, half // sub, flip, jnp.zeros((1, width), jnp.float32))
        db_out_ref[...] = total.astype(jnp.bfloat16)

    def remote_step(step, total):
        block = pl.ds(pl.multiple_of(step * sub, sub), sub)
        parts = []
        for start in range(0, tile, sub):
            cols = slice(start, start + sub)
            value, d_act = act_tile(other_ref[block, :width], other_ref[block, width:], w_in_ref[:, cols], b_in_ref[:, cols].astype(jnp.float32), w_out_ref[cols, :])
            h_ref[block, cols] = value
            a_ref[block, cols] = d_act.astype(jnp.bfloat16)
            parts.append(jnp.sum(d_act, axis=0, keepdims=True))
        return total + jnp.concatenate(parts, axis=1)

    total = lax.fori_loop(0, half // sub, remote_step, dbias_ref[...])
    db_in_ref[...] = total.astype(jnp.bfloat16)

    def grad_step(step, carry):
        cols = pl.ds(pl.multiple_of(step * sub, sub), sub)
        d_in = mm(xt_ref[:, :half], dact_ref[:, cols]) + mm(xt_ref[:, half:], a_ref[:, cols])
        dw_in_ref[:, cols] = d_in.astype(jnp.bfloat16)
        d_out = mm(dt_ref[:, :half], hidden_ref[:, cols]) + mm(dt_ref[:, half:], h_ref[:, cols])
        dw_out_ref[cols, :] = d_out.T.astype(jnp.bfloat16)
        return carry

    lax.fori_loop(0, tile // sub, grad_step, 0)


def grad_call(index, own, other, hidden, dact, dbias, w_in, b_in, w_out, partial_grads, tile=512, sub=256):
    num_rows, wide = own.shape
    experts, width, hidden_size = w_in.shape
    resident = pl.BlockSpec((num_rows, wide), lambda i: (0, 0), pipeline_mode=pl.Buffered(1))
    saved = pl.BlockSpec((num_rows, tile), lambda i: (0, i))
    in_specs = [
        resident,
        resident,
        saved,
        saved,
        pl.BlockSpec((1, tile), lambda i: (0, i)),
        pl.BlockSpec((None, width, tile), lambda i: (index, 0, i)),
        pl.BlockSpec((None, 1, tile), lambda i: (index, 0, i)),
        pl.BlockSpec((None, tile, width), lambda i: (index, i, 0)),
    ]
    operands = [own, other, hidden, dact, dbias, w_in, b_in[:, None, :], w_out]
    aliases = {}
    if partial_grads is not None:
        for place, grad in enumerate(partial_grads):
            aliases[len(operands)] = place
            operands.append(grad)
            in_specs.append(pl.BlockSpec(memory_space=pl.ANY))
    flops = 12 * num_rows * width * hidden_size
    return pl.pallas_call(
        functools.partial(grad_kernel, sub),
        grid=(hidden_size // tile,),
        in_specs=in_specs,
        out_specs=[
            pl.BlockSpec((None, width, tile), lambda i: (index, 0, i)),
            pl.BlockSpec((None, 1, tile), lambda i: (index, 0, i)),
            pl.BlockSpec((None, tile, width), lambda i: (index, i, 0)),
            pl.BlockSpec((None, 1, width), lambda i: (index, 0, 0)),
        ],
        out_shape=[
            jax.ShapeDtypeStruct((experts, width, hidden_size), jnp.bfloat16),
            jax.ShapeDtypeStruct((experts, 1, hidden_size), jnp.bfloat16),
            jax.ShapeDtypeStruct((experts, hidden_size, width), jnp.bfloat16),
            jax.ShapeDtypeStruct((experts, 1, width), jnp.bfloat16),
        ],
        scratch_shapes=[
            pltpu.VMEM((width, 2 * num_rows), jnp.bfloat16),
            pltpu.VMEM((width, 2 * num_rows), jnp.bfloat16),
            pltpu.VMEM((num_rows, tile), jnp.bfloat16),
            pltpu.VMEM((num_rows, tile), jnp.bfloat16),
        ],
        input_output_aliases=aliases,
        compiler_params=pltpu.CompilerParams(dimension_semantics=("arbitrary",), vmem_limit_bytes=60 * 2**20),
        cost_estimate=pl.CostEstimate(flops=flops, bytes_accessed=8 * num_rows * hidden_size, transcendentals=num_rows * hidden_size),
        name="expert_grad",
    )(*operands)


def solution(mesh):
    token_spec = P(ALL_AXES)
    expert_spec = P("ep")
    ep_size = mesh.shape["ep"]

    def local_step(x_loc, modality, router, expert_ids, priority, w_in, b_in, w_out, b_out, dy_loc):
        num_tokens, width = x_loc.shape
        num_experts = router.shape[1]
        local_experts = w_in.shape[0]
        capacity = num_tokens // num_experts
        chunk = ep_size * capacity
        slot_token, token_slot, keep_mask = route_tokens(expert_ids, priority, num_experts, capacity, ep_size)
        log_probs, router_probs, expert_onehot, gate_prob, mod_mask, local_stats = router_forward(x_loc, modality, router, expert_ids)
        stats = lax.psum(local_stats, ALL_AXES)
        aux_loss, mean_probs, mod_count = aux_from_stats(stats, num_experts)
        dy_f32 = dy_loc.astype(jnp.float32)
        d_ytok = (gate_prob[:, None] * dy_f32).astype(jnp.bfloat16)
        source = jnp.pad(jnp.concatenate([x_loc, d_ytok], axis=1), ((0, PAD_ROWS), (0, 0)))

        source, aux_loss = lax.optimization_barrier((source, aux_loss))

        own, other = [], []
        for j in range(local_experts):
            send = source[slot_token[j * chunk:(j + 1) * chunk]].reshape(ep_size, capacity, 2 * width)
            got = lax.all_to_all(send, "ep", 0, 0, tiled=True).reshape(chunk, 2 * width)
            own.append(got)
            other.append(lax.ppermute(got, "dp", [(0, 1), (1, 0)]))
        back = []
        kept = []
        for j in range(local_experts):
            both, hidden, d_act, d_bias = own_call(j, own[j], w_in, b_in, w_out, b_out)
            back.append(lax.all_to_all(both.reshape(ep_size, capacity, 2 * width), "ep", 0, 0, tiled=True).reshape(chunk, 2 * width))
            kept.append((hidden, d_act, d_bias))
        expert_grads = None
        for j in range(local_experts):
            expert_grads = grad_call(j, own[j], other[j], *kept[j], w_in, b_in, w_out, expert_grads)
        d_w_in, d_b_in, d_w_out, d_b_out = expert_grads
        expert_grads = (d_w_in, d_b_in[:, 0], d_w_out, d_b_out[:, 0])

        tok_rows = jnp.concatenate(back, axis=0)[token_slot]
        keep_col = keep_mask[:, None]
        y_tok = tok_rows[:, :width].astype(jnp.float32)
        out_tokens = jnp.where(keep_col, gate_prob[:, None] * y_tok, 0.0).astype(jnp.bfloat16)
        d_gate = jnp.where(keep_mask, jnp.sum(dy_f32 * y_tok, axis=-1), 0.0)
        dx_expert = jnp.where(keep_col, tok_rows[:, width:], 0).astype(jnp.bfloat16)
        d_router_part, dx_router = router_backward(x_loc, router, log_probs, router_probs, expert_onehot, mod_mask, mean_probs, mod_count, d_gate)
        d_router = lax.psum(d_router_part, ALL_AXES)
        return (out_tokens, aux_loss, dx_expert + dx_router, d_router) + tuple(expert_grads)

    return jax.shard_map(
        local_step,
        mesh=mesh,
        in_specs=(token_spec, token_spec, P(), token_spec, token_spec, expert_spec, expert_spec, expert_spec, expert_spec, token_spec),
        out_specs=(token_spec, P(), token_spec, P(), expert_spec, expert_spec, expert_spec, expert_spec),
        check_vma=False,
    )
```

```python
import functools

import jax
import jax.numpy as jnp
from jax import lax
from jax.experimental import pallas as pl
from jax.experimental.pallas import tpu as pltpu
from jax.sharding import PartitionSpec as P


ALL_AXES = ("dp", "ep")


def route_tokens(expert_ids, priority, num_experts, capacity, ep_size):
    num_tokens = expert_ids.shape[0]
    local_experts = num_experts // ep_size
    num_slots = num_experts * capacity
    token_iota = jnp.arange(num_tokens, dtype=jnp.int32)
    slot_iota = jnp.arange(num_slots, dtype=jnp.int32)
    span = num_tokens + capacity
    key_tok = expert_ids * span + priority
    key_fill = (slot_iota // capacity) * span + num_tokens + slot_iota % capacity
    item = jnp.concatenate([token_iota, jnp.full((num_slots,), num_tokens, jnp.int32)])
    sorted_key, sorted_item = lax.sort((jnp.concatenate([key_tok, key_fill]), item), num_keys=1, is_stable=False)
    expert_range = jnp.arange(num_experts, dtype=jnp.int32)
    counts = jnp.sum((expert_ids[:, None] == expert_range[None, :]).astype(jnp.int32), axis=0) + capacity
    expert_of = sorted_key // span
    begin = jnp.sum(jnp.where(expert_range[:, None] < expert_of[None, :], counts[:, None], 0), axis=0)
    position = jnp.arange(num_tokens + num_slots, dtype=jnp.int32) - begin
    keep = position < capacity
    slot = ((expert_of % local_experts) * ep_size + expert_of // local_experts) * capacity + jnp.minimum(position, capacity - 1)
    spread = jnp.where(keep, slot, num_slots)
    _, slot_item = lax.sort((spread, sorted_item), num_keys=1, is_stable=False)
    slot_token = slot_item[:num_slots]
    code = slot * 2 + keep.astype(jnp.int32)
    _, token_code = lax.sort((sorted_item, code), num_keys=1, is_stable=False)
    token_code = token_code[:num_tokens]
    return slot_token, token_code // 2, (token_code % 2) == 1


TOKEN_BLOCK = 1024
STATS_ROWS = 256


def split_three(value):
    high = value.astype(jnp.bfloat16)
    rest = value - high.astype(jnp.float32)
    mid = rest.astype(jnp.bfloat16)
    low = (rest - mid.astype(jnp.float32)).astype(jnp.bfloat16)
    return high, mid, low


def router_columns(x_rows, router_t):
    experts = router_t.shape[0]
    parts = mm(jnp.concatenate(split_three(router_t), axis=0), x_rows, NT)
    logits = parts[:experts] + (parts[experts:2 * experts] + parts[2 * experts:])
    shifted = logits - jnp.max(logits, axis=0, keepdims=True)
    log_probs = shifted - jnp.log(jnp.sum(jnp.exp(shifted), axis=0, keepdims=True))
    return log_probs, jnp.exp(log_probs)


def one_hot_columns(expert_row, experts):
    return lax.broadcasted_iota(jnp.int32, (experts, expert_row.shape[1]), 0) == expert_row


def column_of(row, width):
    turned = jnp.broadcast_to(row, (128, row.shape[1])).T
    return jnp.concatenate([turned] * (width // 128), axis=1)


def lane_fold(value):
    total = value[:, :128]
    for start in range(128, value.shape[1], 128):
        total = total + value[:, start:start + 128]
    return total


def source_kernel(last, x_ref, dy_ref, expert_ref, modality_ref, router_ref, source_ref, stats_ref):
    experts, width = router_ref.shape

    @pl.when(pl.program_id(0) == 0)
    def _():
        stats_ref[...] = jnp.zeros_like(stats_ref)

    @pl.when(pl.program_id(0) < last)
    def _():
        x_rows = x_ref[...]
        log_probs, probs = router_columns(x_rows, router_ref[...])
        gate = jnp.sum(jnp.where(one_hot_columns(expert_ref[...], experts), probs, 0.0), axis=0, keepdims=True)
        source_ref[:, :width] = x_rows
        source_ref[:, width:] = (column_of(gate, width) * dy_ref[...].astype(jnp.float32)).astype(jnp.bfloat16)
        entropy = -jnp.sum(probs * log_probs, axis=0, keepdims=True)
        for kind in range(2):
            chosen = modality_ref[...] == kind
            stats_ref[kind * experts:(kind + 1) * experts, :] += lane_fold(jnp.where(chosen, probs, 0.0))
            row = 2 * experts + kind * 8
            stats_ref[row:row + 1, :] += lane_fold(jnp.where(chosen, entropy, 0.0))
            row = row + 16
            stats_ref[row:row + 1, :] += lane_fold(jnp.where(chosen, 1.0, 0.0))

    @pl.when(pl.program_id(0) == last)
    def _():
        source_ref[...] = jnp.zeros_like(source_ref)


def source_call(x_loc, dy_loc, expert_ids, modality, router_t):
    num_tokens, width = x_loc.shape
    experts = router_t.shape[0]
    last = num_tokens // TOKEN_BLOCK
    held = lambda i: jnp.minimum(i, last - 1)
    rows = pl.BlockSpec((TOKEN_BLOCK, width), lambda i: (held(i), 0))
    line = pl.BlockSpec((None, 1, TOKEN_BLOCK), lambda i: (held(i), 0, 0))
    return pl.pallas_call(
        functools.partial(source_kernel, last),
        grid=(last + 1,),
        in_specs=[rows, rows, line, line, pl.BlockSpec((experts, width), lambda i: (0, 0))],
        out_specs=[pl.BlockSpec((TOKEN_BLOCK, 2 * width), lambda i: (i, 0)), pl.BlockSpec((STATS_ROWS, 128), lambda i: (0, 0))],
        out_shape=[jax.ShapeDtypeStruct((num_tokens + TOKEN_BLOCK, 2 * width), jnp.bfloat16), jax.ShapeDtypeStruct((STATS_ROWS, 128), jnp.float32)],
        compiler_params=pltpu.CompilerParams(dimension_semantics=("arbitrary",)),
        cost_estimate=pl.CostEstimate(flops=200 * num_tokens * width, bytes_accessed=8 * num_tokens * width, transcendentals=0),
        name="router_source",
    )(x_loc, dy_loc, expert_ids.reshape(last, 1, TOKEN_BLOCK), modality.reshape(last, 1, TOKEN_BLOCK), router_t)


def aux_from_stats(stats, experts):
    sums = jnp.sum(stats, axis=1)
    mod_count = jnp.stack([sums[2 * experts + 16], sums[2 * experts + 24]])
    entropy = jnp.stack([sums[2 * experts], sums[2 * experts + 8]])
    mean_probs = sums[:2 * experts].reshape(2, experts) / mod_count[:, None]
    aux_loss = jnp.sum(entropy / mod_count) + jnp.sum(mean_probs * jnp.log(mean_probs))
    return aux_loss, mean_probs, mod_count


def final_kernel(x_ref, dy_ref, got_ref, expert_ref, modality_ref, keep_ref, router_ref, slope_ref, scale_ref, out_ref, dx_ref, d_router_ref):
    experts, width = router_ref.shape
    count = x_ref.shape[0]

    @pl.when(pl.program_id(0) == 0)
    def _():
        d_router_ref[...] = jnp.zeros_like(d_router_ref)

    x_rows = x_ref[...]
    router_t = router_ref[...]
    log_probs, probs = router_columns(x_rows, router_t)
    hot = one_hot_columns(expert_ref[...], experts)
    gate = jnp.sum(jnp.where(hot, probs, 0.0), axis=0, keepdims=True)
    keep_row = keep_ref[...] > 0
    keep_col = column_of(keep_ref[...].astype(jnp.float32), width) > 0.5
    y_rows = got_ref[:, :width].astype(jnp.float32)
    dy_rows = dy_ref[...].astype(jnp.float32)
    out_ref[...] = jnp.where(keep_col, column_of(gate, width) * y_rows, 0.0).astype(jnp.bfloat16)
    d_gate = jnp.where(keep_row, jnp.sum(lane_fold(dy_rows * y_rows).T, axis=0, keepdims=True), 0.0)
    first = modality_ref[...] == 0
    tiles = count // 128
    spread = lambda part: jnp.concatenate([part] * tiles, axis=1)
    global_part = jnp.where(first, spread(slope_ref[:experts]), spread(slope_ref[experts:]))
    inv_count = jnp.where(first, spread(scale_ref[0:1]), spread(scale_ref[8:9]))
    d_probs = jnp.where(hot, d_gate, 0.0) + global_part - log_probs * inv_count
    d_logits = probs * (d_probs - jnp.sum(d_probs * probs, axis=0, keepdims=True))
    high, mid, low = split_three(d_logits)
    parts = mm(jnp.concatenate([high, mid, low], axis=0), x_rows)
    d_router_ref[...] += parts[:experts] + (parts[experts:2 * experts] + parts[2 * experts:])
    r_high, r_mid, r_low = split_three(router_t)
    left = jnp.concatenate([high, high, mid, high, low, mid], axis=0).T
    right = jnp.concatenate([r_high, r_mid, r_high, r_low, r_high, r_mid], axis=0)
    dx_router = mm(left, right).astype(jnp.bfloat16).astype(jnp.float32)
    dx_ref[...] = (jnp.where(keep_col, got_ref[:, width:].astype(jnp.float32), 0.0) + dx_router).astype(jnp.bfloat16)


def final_call(x_loc, dy_loc, got, expert_ids, modality, keep_mask, router_t, mean_probs, mod_count):
    num_tokens, width = x_loc.shape
    experts = router_t.shape[0]
    blocks = num_tokens // TOKEN_BLOCK
    slope = jnp.broadcast_to((jnp.log(mean_probs) / mod_count[:, None]).reshape(2 * experts, 1), (2 * experts, 128))
    scale = jnp.broadcast_to(jnp.repeat(1.0 / mod_count, 8)[:, None], (16, 128))
    rows = pl.BlockSpec((TOKEN_BLOCK, width), lambda i: (i, 0))
    line = pl.BlockSpec((None, 1, TOKEN_BLOCK), lambda i: (i, 0, 0))
    fixed = lambda shape: pl.BlockSpec(shape, lambda i: (0, 0))
    as_lines = lambda value: value.astype(jnp.int32).reshape(blocks, 1, TOKEN_BLOCK)
    return pl.pallas_call(
        final_kernel,
        grid=(blocks,),
        in_specs=[rows, rows, pl.BlockSpec((TOKEN_BLOCK, 2 * width), lambda i: (i, 0)), line, line, line, fixed((experts, width)), fixed((2 * experts, 128)), fixed((16, 128))],
        out_specs=[rows, rows, fixed((experts, width))],
        out_shape=[
            jax.ShapeDtypeStruct((num_tokens, width), jnp.bfloat16),
            jax.ShapeDtypeStruct((num_tokens, width), jnp.bfloat16),
            jax.ShapeDtypeStruct((experts, width), jnp.float32),
        ],
        compiler_params=pltpu.CompilerParams(dimension_semantics=("arbitrary",)),
        cost_estimate=pl.CostEstimate(flops=1000 * num_tokens * width, bytes_accessed=12 * num_tokens * width, transcendentals=0),
        name="router_final",
    )(x_loc, dy_loc, got, as_lines(expert_ids), as_lines(modality), as_lines(keep_mask), router_t, slope, scale)


def mm(lhs, rhs, dims=(((1,), (0,)), ((), ()))):
    return lax.dot_general(lhs, rhs, dims, preferred_element_type=jnp.float32)


SLOTS = 4
STRIP = 32
GELU_A = 0.7978845608028654
GELU_B = 0.044715 * GELU_A
NT = (((1,), (1,)), ((), ()))


def gelu_and_slope(act):
    sq = act * act
    gate = 0.5 * jnp.tanh(act * (GELU_B * sq + GELU_A)) + 0.5
    value = act * gate
    slope = gate + value * (1.0 - gate) * (6.0 * GELU_B * sq + 2.0 * GELU_A)
    return value, slope


def act_products(unit, act_ref, dh_ref, x_rows, d_rows, w_in, w_out):
    slot = unit % SLOTS
    act_ref[slot] = mm(x_rows, w_in)
    dh_ref[slot] = mm(d_rows, w_out, NT)


def act_finish(unit, act_ref, dh_ref, bias, put):
    slot = unit % SLOTS
    count, cols = act_ref.shape[1:]
    total = jnp.zeros((8, cols), jnp.float32)
    for start in range(0, count, STRIP):
        strip = slice(start, start + STRIP)
        d_hidden = dh_ref[slot, strip].astype(jnp.bfloat16).astype(jnp.float32)
        value, slope = gelu_and_slope(act_ref[slot, strip] + bias)
        d_act = d_hidden * slope
        put(start, value.astype(jnp.bfloat16), d_act.astype(jnp.bfloat16))
        total = total + jnp.sum(d_act.reshape(STRIP // 8, 8, cols), axis=0)
    return total


def act_sweep(units):
    finished = None
    for place, (products, finish) in enumerate(units):
        products(place)
        if finished is not None:
            finished(place - 1)
        finished = finish
    finished(len(units) - 1)


def own_kernel(sub, rows_ref, w_in_ref, b_in_ref, w_out_ref, b_out_ref, both_ref, hidden_ref, dact_ref, dbias_ref, act_ref, dh_ref):
    count = rows_ref.shape[0]
    width = w_in_ref.shape[0]
    hidden_size = w_in_ref.shape[1]

    @pl.when(pl.program_id(0) == 0)
    def _():
        dbias_ref[...] = jnp.zeros_like(dbias_ref)

    def unit(col, start):
        cols = slice(col, col + sub)
        block = slice(start, start + sub)

        def products(place):
            act_products(place, act_ref, dh_ref, rows_ref[block, :width], rows_ref[block, width:], w_in_ref[:, cols], w_out_ref[cols, :])

        def finish(place):
            def put(row, value, d_act):
                hidden_ref[start + row:start + row + STRIP, cols] = value
                dact_ref[start + row:start + row + STRIP, cols] = d_act

            total = act_finish(place, act_ref, dh_ref, b_in_ref[:, cols].astype(jnp.float32), put)
            dbias_ref[:, cols] += jnp.sum(total, axis=0, keepdims=True)

        return products, finish

    act_sweep([unit(col, start) for col in range(0, hidden_size, sub) for start in range(0, count, sub)])

    def out_step(step, carry):
        cols = pl.ds(pl.multiple_of(step * sub, sub), sub)
        back = pl.ds(pl.multiple_of(width + step * sub, sub), sub)
        both_ref[:, cols] = (mm(hidden_ref[...], w_out_ref[:, cols]) + b_out_ref[:, cols].astype(jnp.float32)).astype(jnp.bfloat16)
        both_ref[:, back] = mm(dact_ref[...], w_in_ref[cols, :], NT).astype(jnp.bfloat16)
        return carry

    lax.fori_loop(0, width // sub, out_step, 0)


def own_call(index, rows, w_in, b_in, w_out, b_out, block=512, sub=256):
    num_rows, wide = rows.shape
    width = wide // 2
    hidden_size = w_in.shape[2]
    whole = lambda shape: pl.BlockSpec((None,) + shape, lambda i: (index, 0, 0), pipeline_mode=pl.Buffered(1))
    flops = 8 * num_rows * width * hidden_size
    return pl.pallas_call(
        functools.partial(own_kernel, sub),
        grid=(num_rows // block,),
        in_specs=[
            pl.BlockSpec((block, wide), lambda i: (i, 0)),
            whole((width, hidden_size)),
            whole((1, hidden_size)),
            whole((hidden_size, width)),
            whole((1, width)),
        ],
        out_specs=[
            pl.BlockSpec((block, wide), lambda i: (i, 0)),
            pl.BlockSpec((block, hidden_size), lambda i: (i, 0)),
            pl.BlockSpec((block, hidden_size), lambda i: (i, 0)),
            pl.BlockSpec((1, hidden_size), lambda i: (0, 0)),
        ],
        out_shape=[
            jax.ShapeDtypeStruct((num_rows, wide), jnp.bfloat16),
            jax.ShapeDtypeStruct((num_rows, hidden_size), jnp.bfloat16),
            jax.ShapeDtypeStruct((num_rows, hidden_size), jnp.bfloat16),
            jax.ShapeDtypeStruct((1, hidden_size), jnp.float32),
        ],
        scratch_shapes=[pltpu.VMEM((SLOTS, sub, sub), jnp.float32), pltpu.VMEM((SLOTS, sub, sub), jnp.float32)],
        compiler_params=pltpu.CompilerParams(dimension_semantics=("arbitrary",), vmem_limit_bytes=60 * 2**20),
        cost_estimate=pl.CostEstimate(flops=flops, bytes_accessed=8 * num_rows * hidden_size, transcendentals=num_rows * hidden_size),
        name="expert_own",
    )(rows, w_in, b_in[:, None, :], w_out, b_out[:, None, :])


def grad_kernel(sub, own_ref, other_ref, hidden_ref, dact_ref, dbias_ref, w_in_ref, b_in_ref, w_out_ref, *refs):
    dw_in_ref, db_in_ref, dw_out_ref, db_out_ref, xt_ref, dt_ref, h_ref, a_ref, act_ref, dh_ref = refs[-10:]
    half = own_ref.shape[0]
    width = own_ref.shape[1] // 2
    tile = w_in_ref.shape[1]

    @pl.when(pl.program_id(0) == 0)
    def _():
        def flip(step, total):
            for ref, base in ((own_ref, 0), (other_ref, half)):
                block = pl.ds(pl.multiple_of(step * sub, sub), sub)
                cols = pl.ds(pl.multiple_of(base + step * sub, sub), sub)
                d_rows = ref[block, width:]
                xt_ref[:, cols] = ref[block, :width].T
                dt_ref[:, cols] = d_rows.T
                total = total + jnp.sum(d_rows.astype(jnp.float32), axis=0, keepdims=True)
            return total

        total = lax.fori_loop(0, half // sub, flip, jnp.zeros((1, width), jnp.float32))
        db_out_ref[...] = total.astype(jnp.bfloat16)

    totals = {}

    def unit(col, start):
        cols = slice(col, col + sub)
        block = slice(start, start + sub)

        def products(place):
            act_products(place, act_ref, dh_ref, other_ref[block, :width], other_ref[block, width:], w_in_ref[:, cols], w_out_ref[cols, :])

        def finish(place):
            def put(row, value, d_act):
                h_ref[start + row:start + row + STRIP, cols] = value
                a_ref[start + row:start + row + STRIP, cols] = d_act

            total = act_finish(place, act_ref, dh_ref, b_in_ref[:, cols].astype(jnp.float32), put)
            totals[col] = totals[col] + total if col in totals else total
            if start + sub == half:
                db_in_ref[:, cols] = (dbias_ref[:, cols] + jnp.sum(totals[col], axis=0, keepdims=True)).astype(jnp.bfloat16)

        return products, finish

    act_sweep([unit(col, start) for col in range(0, tile, sub) for start in range(0, half, sub)])

    def grad_step(step, carry):
        cols = pl.ds(pl.multiple_of(step * sub, sub), sub)
        d_in = mm(xt_ref[:, :half], dact_ref[:, cols]) + mm(xt_ref[:, half:], a_ref[:, cols])
        dw_in_ref[:, cols] = d_in.astype(jnp.bfloat16)
        d_out = mm(dt_ref[:, :half], hidden_ref[:, cols]) + mm(dt_ref[:, half:], h_ref[:, cols])
        dw_out_ref[cols, :] = d_out.T.astype(jnp.bfloat16)
        return carry

    lax.fori_loop(0, tile // sub, grad_step, 0)


def grad_call(index, own, other, hidden, dact, dbias, w_in, b_in, w_out, partial_grads, tile=256, sub=256):
    num_rows, wide = own.shape
    experts, width, hidden_size = w_in.shape
    resident = pl.BlockSpec((num_rows, wide), lambda i: (0, 0), pipeline_mode=pl.Buffered(1))
    saved = pl.BlockSpec((num_rows, tile), lambda i: (0, i))
    in_specs = [
        resident,
        resident,
        saved,
        saved,
        pl.BlockSpec((1, tile), lambda i: (0, i)),
        pl.BlockSpec((None, width, tile), lambda i: (index, 0, i)),
        pl.BlockSpec((None, 1, tile), lambda i: (index, 0, i)),
        pl.BlockSpec((None, tile, width), lambda i: (index, i, 0)),
    ]
    operands = [own, other, hidden, dact, dbias, w_in, b_in[:, None, :], w_out]
    aliases = {}
    if partial_grads is not None:
        for place, grad in enumerate(partial_grads):
            aliases[len(operands)] = place
            operands.append(grad)
            in_specs.append(pl.BlockSpec(memory_space=pl.ANY))
    flops = 12 * num_rows * width * hidden_size
    return pl.pallas_call(
        functools.partial(grad_kernel, sub),
        grid=(hidden_size // tile,),
        in_specs=in_specs,
        out_specs=[
            pl.BlockSpec((None, width, tile), lambda i: (index, 0, i)),
            pl.BlockSpec((None, 1, tile), lambda i: (index, 0, i)),
            pl.BlockSpec((None, tile, width), lambda i: (index, i, 0)),
            pl.BlockSpec((None, 1, width), lambda i: (index, 0, 0)),
        ],
        out_shape=[
            jax.ShapeDtypeStruct((experts, width, hidden_size), jnp.bfloat16),
            jax.ShapeDtypeStruct((experts, 1, hidden_size), jnp.bfloat16),
            jax.ShapeDtypeStruct((experts, hidden_size, width), jnp.bfloat16),
            jax.ShapeDtypeStruct((experts, 1, width), jnp.bfloat16),
        ],
        scratch_shapes=[
            pltpu.VMEM((width, 2 * num_rows), jnp.bfloat16),
            pltpu.VMEM((width, 2 * num_rows), jnp.bfloat16),
            pltpu.VMEM((num_rows, tile), jnp.bfloat16),
            pltpu.VMEM((num_rows, tile), jnp.bfloat16),
            pltpu.VMEM((SLOTS, sub, sub), jnp.float32),
            pltpu.VMEM((SLOTS, sub, sub), jnp.float32),
        ],
        input_output_aliases=aliases,
        compiler_params=pltpu.CompilerParams(dimension_semantics=("arbitrary",), vmem_limit_bytes=60 * 2**20),
        cost_estimate=pl.CostEstimate(flops=flops, bytes_accessed=8 * num_rows * hidden_size, transcendentals=num_rows * hidden_size),
        name="expert_grad",
    )(*operands)


def solution(mesh):
    token_spec = P(ALL_AXES)
    expert_spec = P("ep")
    ep_size = mesh.shape["ep"]

    def local_step(x_loc, modality, router, expert_ids, priority, w_in, b_in, w_out, b_out, dy_loc):
        num_tokens, width = x_loc.shape
        num_experts = router.shape[1]
        local_experts = w_in.shape[0]
        capacity = num_tokens // num_experts
        chunk = ep_size * capacity
        slot_token, token_slot, keep_mask = route_tokens(expert_ids, priority, num_experts, capacity, ep_size)
        router_t = router.T
        source, local_stats = source_call(x_loc, dy_loc, expert_ids, modality, router_t)
        stats = lax.psum(local_stats, ALL_AXES)
        aux_loss, mean_probs, mod_count = aux_from_stats(stats, num_experts)

        own, other = [], []
        for j in range(local_experts):
            send = source[slot_token[j * chunk:(j + 1) * chunk]].reshape(ep_size, capacity, 2 * width)
            got = lax.all_to_all(send, "ep", 0, 0, tiled=True).reshape(chunk, 2 * width)
            own.append(got)
            other.append(lax.ppermute(got, "dp", [(0, 1), (1, 0)]))
        back = []
        kept = []
        for j in range(local_experts):
            both, hidden, d_act, d_bias = own_call(j, own[j], w_in, b_in, w_out, b_out)
            back.append(lax.all_to_all(both.reshape(ep_size, capacity, 2 * width), "ep", 0, 0, tiled=True).reshape(chunk, 2 * width))
            kept.append((hidden, d_act, d_bias))
        expert_grads = None
        for j in range(local_experts):
            expert_grads = grad_call(j, own[j], other[j], *kept[j], w_in, b_in, w_out, expert_grads)
        d_w_in, d_b_in, d_w_out, d_b_out = expert_grads
        expert_grads = (d_w_in, d_b_in[:, 0], d_w_out, d_b_out[:, 0])

        got = jnp.concatenate(back, axis=0)[token_slot]
        out_tokens, dx_tokens, d_router_part = final_call(x_loc, dy_loc, got, expert_ids, modality, keep_mask, router_t, mean_probs, mod_count)
        d_router = lax.psum(d_router_part, ALL_AXES).T
        return (out_tokens, aux_loss, dx_tokens, d_router) + tuple(expert_grads)

    return jax.shard_map(
        local_step,
        mesh=mesh,
        in_specs=(token_spec, token_spec, P(), token_spec, token_spec, expert_spec, expert_spec, expert_spec, expert_spec, token_spec),
        out_specs=(token_spec, P(), token_spec, P(), expert_spec, expert_spec, expert_spec, expert_spec),
        check_vma=False,
    )
```
